32 devices in a mesh: dp: 4 (over y, x), fsdp: 8 (over z, core).
Axes of the slice: x: 2, y: 2, z: 4, core: 2. Of those that a mesh axis runs over, the one named last changes fastest.
Arguments:
- tokens: bfloat16 [96, 257, 1408], P(('dp', 'fsdp')), parts along dimension 0, may hold values from -16 to 16
- ln1_gain: float32 [1408], replicated, may hold values from 0.1 to 1.9
- ln1_bias: float32 [1408], replicated, may hold values from -3 to 3
- qkv_weight: bfloat16 [1408, 4224], P('fsdp'), may hold values from -3 to 3
- qkv_bias: float32 [4224], replicated, may hold values from -3 to 3
- proj_weight: bfloat16 [1408, 1408], P('fsdp'), may hold values from -0.15625 to 0.15625
- proj_bias: float32 [1408], replicated, may hold values from -3 to 3
- ln2_gain: float32 [1408], replicated, may hold values from 0.1 to 1.9
- ln2_bias: float32 [1408], replicated, may hold values from -3 to 3
- fc1_weight: bfloat16 [1408, 3072], P('fsdp'), may hold values from -0.15625 to 0.15625
- fc1_bias: float32 [3072], replicated, may hold values from -3 to 3
- fc2_weight: bfloat16 [3072, 1408], P('fsdp'), may hold values from -0.109375 to 0.109375
- fc2_bias: float32 [1408], replicated, may hold values from -3 to 3
Outputs:
- layer_out: bfloat16 [96, 257, 1408], P(('dp', 'fsdp')), parts along dimension 0
The draws below stay inside these ranges and needn't reach their ends.
There are 4 independent parts, one for each index of `dp`. The reference program is written for one: setup_inputs(seed, part) draws one part's arguments, and reference() takes and returns one part's arrays. A program takes and returns all parts, laid end to end along the dimension named above; an argument that names none is the same for every part. Nothing has to cross between parts.
All inputs are finite; a program needn't handle non-finite values.
Results may differ from the reference program's by a relative error of at most 0.0045.
Values may be sent and summed in bfloat16 or wider, within the bound.
A program may use at most 448 MiB of HBM per device.

```python
import math
import jax
import jax.numpy as jnp
from jax import lax

D = 1408
HEADS = 16
HEAD_DIM = 88
FF = 3072
SEQ = 257
IMAGES = 24


def draw_tokens(key, part):
    base_key = jax.random.fold_in(key, 11)
    first, second = jax.random.split(base_key, 2)
    values = jax.random.normal(first, (IMAGES, SEQ, D), jnp.float32)
    row_scale = jnp.exp(jax.random.uniform(second, (IMAGES, SEQ, 1), jnp.float32, math.log(0.5), math.log(8.0)))
    values = jnp.clip(values * row_scale, -16.0, 16.0)
    return values.astype(jnp.bfloat16)


def draw_qkv_weight(key, part):
    base_key = jax.random.fold_in(key, 23)
    values = jax.random.normal(base_key, (D, 3 * D), jnp.float32) * D ** (-0.5)
    values = jnp.clip(values, -3.0, 3.0)
    return values.astype(jnp.bfloat16)


def levels(rng, shape, pieces, low, top_value):
    factor_of = 1.0
    for axis_at, parts in pieces:
        steps = jax.random.uniform(jax.random.fold_in(jax.random.fold_in(rng, 6), axis_at), (parts,), jnp.float32, low / len(pieces), top_value / len(pieces))
        factor_of = factor_of * jnp.repeat(jnp.exp(steps), shape[axis_at] // parts).reshape((-1,) + (1,) * (len(shape) - 1 - axis_at))
    return factor_of


def normal_values(key, extent, width, reach, cuts=(), held_as=jnp.bfloat16):
    factor_of = levels(key, extent, cuts, -0.22, 0.18) if cuts else 1.0
    entries = jax.random.normal(key, extent, jnp.float32) * width * factor_of
    return jnp.minimum(jnp.maximum(entries, -reach), reach).astype(held_as)


def setup_inputs(seed: int = 0, part: int = 0) -> dict:
    splits = jax.random.split(jax.random.key(seed), 14)
    own_keys = jax.random.split(jax.random.fold_in(splits[13], part), 14)
    return {
        "tokens": draw_tokens(jax.random.fold_in(jax.random.fold_in(splits[13], part), 71), part),
        "ln1_gain": jnp.clip(1.0 + 0.18 * jax.random.normal(splits[1], (D,), jnp.float32), 0.1, 1.9),
        "ln1_bias": normal_values(splits[2], (D,), 0.5, 3.0, (), jnp.float32),
        "qkv_weight": draw_qkv_weight(jax.random.fold_in(splits[13], 71), part),
        "qkv_bias": normal_values(splits[4], (3 * D,), 0.5, 3.0, (), jnp.float32),
        "proj_weight": normal_values(splits[5], (D, D), D ** -0.5, 0.15625, ((0, 8),)),
        "proj_bias": normal_values(splits[6], (D,), 0.5, 3.0, (), jnp.float32),
        "ln2_gain": jnp.clip(1.0 + 0.18 * jax.random.normal(splits[7], (D,), jnp.float32), 0.1, 1.9),
        "ln2_bias": normal_values(splits[8], (D,), 0.5, 3.0, (), jnp.float32),
        "fc1_weight": normal_values(splits[9], (D, FF), D ** -0.5, 0.15625, ((0, 8),)),
        "fc1_bias": normal_values(splits[10], (FF,), 0.5, 3.0, (), jnp.float32),
        "fc2_weight": normal_values(splits[11], (FF, D), FF ** -0.5, 0.109375, ((0, 8),)),
        "fc2_bias": normal_values(splits[12], (D,), 0.5, 3.0, (), jnp.float32),
    }


def layer_norm(values, gain, bias):
    average = lax.optimization_barrier(jnp.mean(values, axis=-1, keepdims=True))
    centered = values - average
    variance = lax.optimization_barrier(jnp.mean(centered * centered, axis=-1, keepdims=True))
    return centered * lax.rsqrt(variance + 1e-06) * gain + bias

def reference(tokens, ln1_gain, ln1_bias, qkv_weight, qkv_bias, proj_weight, proj_bias, ln2_gain, ln2_bias, fc1_weight, fc1_bias, fc2_weight, fc2_bias):
    flat_rows = tokens.reshape(-1, D).astype(jnp.float32)
    normed = layer_norm(flat_rows, ln1_gain, ln1_bias).astype(jnp.bfloat16)
    qkv_proj = (jnp.dot(normed, qkv_weight, preferred_element_type=jnp.float32) + qkv_bias).astype(jnp.bfloat16)
    qkv_proj = qkv_proj.reshape(IMAGES, SEQ, 3, HEADS, HEAD_DIM)
    score_scale = HEAD_DIM ** (-0.5)

    def attend(image):
        queries = image[:, 0].astype(jnp.float32)
        key_part = image[:, 1].astype(jnp.float32)
        value_part = image[:, 2].astype(jnp.float32)
        scores = jnp.einsum('qhd,khd->hqk', queries, key_part) * score_scale
        probs = jax.nn.softmax(scores, axis=-1).astype(jnp.bfloat16)
        mixed = jnp.einsum('hqk,khd->qhd', probs.astype(jnp.float32), value_part)
        return mixed.astype(jnp.bfloat16).reshape(SEQ, D)
    attended = lax.map(attend, qkv_proj).reshape(-1, D)
    resid = jnp.dot(attended, proj_weight, preferred_element_type=jnp.float32) + proj_bias + flat_rows
    normed_two = layer_norm(resid, ln2_gain, ln2_bias).astype(jnp.bfloat16)
    hidden = jax.nn.gelu(jnp.dot(normed_two, fc1_weight, preferred_element_type=jnp.float32) + fc1_bias, approximate=False).astype(jnp.bfloat16)
    result = jnp.dot(hidden, fc2_weight, preferred_element_type=jnp.float32) + fc2_bias + resid
    return result.astype(jnp.bfloat16).reshape(IMAGES, SEQ, D)
```

```python
import functools
import math
import jax
import jax.numpy as jnp
from jax import lax
from jax.experimental import pallas as pl
from jax.experimental.pallas import tpu as pltpu
from jax.sharding import PartitionSpec as P

HEADS = 16
LANES = 128
PACK = 16
EPS = 1e-06


def layer_norm(values, gain, bias):
    average = jnp.mean(values, axis=-1, keepdims=True)
    centered = values - average
    variance = jnp.mean(centered * centered, axis=-1, keepdims=True)
    return centered * lax.rsqrt(variance + EPS) * gain + bias


def product(left, weight):
    return jnp.dot(left, weight, preferred_element_type=jnp.float32)


def round_up(value, step):
    return -(-value // step) * step


def row_block(rows, most):
    best = PACK
    for size in range(PACK, most + 1, PACK):
        if rows % size == 0:
            best = size
    return best


class Plan:
    def __init__(self, shares, ring, tokens, weights):
        self.shares, self.ring = shares, ring
        self.images, self.seq, self.width = tokens.shape
        qkv, proj, fc1, fc2 = weights
        self.depth = qkv.shape[0]
        self.deep = fc2.shape[0]
        self.wide = [w.shape[1] for w in (qkv, proj, fc1)]
        self.total = sum(self.wide)
        self.chunk = shares * LANES
        self.hidden = fc1.shape[1]
        self.seq_pad = round_up(self.seq, PACK)
        self.rows = self.images * self.seq_pad
        self.fits = (
            shares == 4
            and ring % 2 == 0
            and ring >= 4
            and self.depth % PACK == 0
            and self.depth >= 2 * PACK
            and self.deep % (shares * PACK) == 0
            and self.deep // shares >= 2 * PACK
            and all(w % LANES == 0 for w in self.wide)
            and self.total % self.chunk == 0
            and self.width % LANES == 0
        )
        if not self.fits:
            return
        self.narrow = 2 * LANES
        self.col_chunks = self.total // self.chunk
        self.kinds = [("col", 0, self.col_chunks, self.chunk, 0)]
        whole = self.width // self.narrow
        at = self.col_chunks
        self.kinds.append(("row", at, at + whole, self.narrow, 0))
        at += whole
        if self.width % self.narrow:
            self.kinds.append(("row", at, at + 1, self.width % self.narrow, whole * self.narrow))
            at += 1
        self.chunks = at
        kept = ring * (self.depth * self.total + self.deep * self.width) * 2
        acts = self.rows * (self.width * (4 + 2 + 2 + 2) + max(3 * self.width, self.hidden) * 2)
        self.fits = kept + acts < 58 * 1024 * 1024


def fused_kernel(plan, tokens, qkv_hbm, proj_hbm, fc1_hbm, fc2_hbm,
                 ln1_gain, ln1_bias, qkv_bias, proj_bias, ln2_gain, ln2_bias, fc1_bias, fc2_bias,
                 out, wall, wtwo, tok, resid, normed, qkv, mixed,
                 send_sem, recv_sem, own_sem, out_sem):
    shares, ring = plan.shares, plan.ring
    zs = ring // 2
    depth, deep = plan.depth, plan.deep
    rows, seq, seq_pad = plan.rows, plan.seq, plan.seq_pad
    share = lax.axis_index("dp")
    place = lax.axis_index("fsdp")
    z, core = place // 2, place % 2
    Z, X1, Y1, X2, Y2, PART = range(6)
    side_x = lax.rem(share, 2) * -2 + 1 + share
    side_y = share + 2 - (share // 2) * 4
    partner = z * 2 + 1 - core

    def others():
        for step in range(1, zs):
            yield lax.rem(z + step, zs)

    def device(d, f):
        return {"dp": d, "fsdp": f}

    def part(kind, who, block_share, low, high):
        name, first, _, cols, base = kind[:5]
        g = kind[5]
        if name == "col":
            r = pl.multiple_of(who * depth + low, PACK)
            c = pl.multiple_of((g * shares + block_share) * LANES, LANES)
            return wall.at[pl.ds(r, high - low), pl.ds(c, LANES)]
        size = deep // shares
        r = pl.multiple_of(who * deep + block_share * size + low, PACK)
        c = pl.multiple_of(base + (g - first) * cols, LANES)
        return wtwo.at[pl.ds(r, high - low), pl.ds(c, cols)]

    def entire(kind, who):
        name, first, _, cols, base = kind[:5]
        g = kind[5]
        if name == "col":
            return wall.at[pl.ds(pl.multiple_of(who * depth, PACK), depth),
                           pl.ds(pl.multiple_of(g * cols, LANES), cols)]
        return wtwo.at[pl.ds(pl.multiple_of(who * deep, PACK), deep),
                       pl.ds(pl.multiple_of(base + (g - first) * cols, LANES), cols)]

    def sized(kind, count, part_rows, cols):
        ref = wall if kind[0] == "col" else wtwo
        return ref.at[pl.ds(0, count * part_rows), pl.ds(0, cols)]

    def spans(kind):
        size = depth if kind[0] == "col" else deep // shares
        cut = round_up(size // 2, PACK)
        return size, cut, LANES if kind[0] == "col" else kind[3]

    def copy(ref, phase, g, d, f):
        return pltpu.make_async_remote_copy(
            src_ref=ref, dst_ref=ref, send_sem=send_sem.at[phase, g], recv_sem=recv_sem.at[phase, g],
            device_id=device(d, f), device_id_type=pl.DeviceIdType.MESH)

    def volume(kind, phase):
        size, cut, cols = spans(kind)
        if phase == PART:
            full = depth if kind[0] == "col" else deep
            return sized(kind, zs, full, kind[3])
        part_rows = {Z: size, X1: size, Y1: size, X2: cut, Y2: size - cut}[phase]
        return sized(kind, zs - 1, part_rows, cols)

    def wait_in(kind, phase):
        g = kind[5]
        pltpu.make_async_copy(volume(kind, phase), volume(kind, phase), recv_sem.at[phase, g]).wait()

    def wait_out(kind, phase):
        g = kind[5]
        pltpu.make_async_copy(volume(kind, phase), volume(kind, phase), send_sem.at[phase, g]).wait()

    def each_kind(g, body):
        if isinstance(g, int):
            for kind in plan.kinds:
                if kind[1] <= g < kind[2]:
                    body(kind + (g,))
            return
        for kind in plan.kinds:
            @pl.when(jnp.logical_and(g >= kind[1], g < kind[2]))
            def _(kind=kind):
                body(kind + (g,))

    def send_z(g):
        def body(kind):
            size, _, _ = spans(kind)
            for other in others():
                copy(part(kind, place, share, 0, size), Z, g, share, other * 2 + core).start()
        each_kind(g, body)

    def relay_a(g):
        def body(kind):
            size, _, _ = spans(kind)
            wait_in(kind, Z)
            for other in others():
                block = part(kind, other * 2 + core, share, 0, size)
                copy(block, X1, g, side_x, place).start()
                copy(block, Y1, g, side_y, place).start()
        each_kind(g, body)

    def relay_b(g):
        def body(kind):
            size, cut, _ = spans(kind)
            wait_in(kind, X1)
            wait_in(kind, Y1)
            for other in others():
                who = other * 2 + core
                copy(part(kind, who, side_y, 0, cut), X2, g, side_x, place).start()
                copy(part(kind, who, side_x, cut, size), Y2, g, side_y, place).start()
        each_kind(g, body)

    def relay_c(g):
        def body(kind):
            wait_in(kind, X2)
            wait_in(kind, Y2)
            for who in range(zs):
                copy(entire(kind, who * 2 + core), PART, g, share, partner).start()
        each_kind(g, body)

    def finish(g):
        each_kind(g, lambda kind: wait_in(kind, PART))

    ahead = 4

    def tick(t):
        if isinstance(t, int):
            for low, action in ((ahead, send_z), (0, relay_a), (-1, relay_b), (-2, relay_c)):
                if 0 <= t + low < plan.chunks:
                    action(t + low)
            return
        send_z(t + ahead)
        relay_a(t)
        relay_b(t - 1)
        relay_c(t - 2)

    token_copy = pltpu.make_async_copy(tokens, tok, own_sem.at[4])
    token_copy.start()
    base = 0
    own = []
    for at, (ref, cols) in enumerate(zip((qkv_hbm, proj_hbm, fc1_hbm), plan.wide)):
        own.append(pltpu.make_async_copy(
            ref, wall.at[pl.ds(pl.multiple_of(place * depth, PACK), depth), pl.ds(base, cols)], own_sem.at[at]))
        base += cols
    own.append(pltpu.make_async_copy(
        fc2_hbm, wtwo.at[pl.ds(pl.multiple_of(place * deep, PACK), deep), :], own_sem.at[3]))
    for c in own:
        c.start()

    barrier = pltpu.get_barrier_semaphore()
    peers = [(share, other * 2 + core) for other in others()]
    peers += [(side_x, place), (side_y, place), (share, partner)]
    for d, f in peers:
        pl.semaphore_signal(barrier, inc=1, device_id=device(d, f), device_id_type=pl.DeviceIdType.MESH)
    pl.semaphore_wait(barrier, len(peers))
    for c in own:
        c.wait()
    for g in range(ahead):
        send_z(g)

    token_copy.wait()
    resid[...] = jnp.zeros_like(resid)
    for i in range(plan.images):
        resid[pl.ds(i * seq_pad, seq), :] = tok[i].astype(jnp.float32)
    block = row_block(rows, 64)

    def norm(gain, bias):
        def body(r, carry):
            at = pl.ds(pl.multiple_of(r * block, PACK), block)
            normed[at, :] = layer_norm(resid[at, :], gain[...], bias[...]).astype(jnp.bfloat16)
            return carry
        lax.fori_loop(0, rows // block, body, 0)

    norm(ln1_gain, ln1_bias)

    qkv_cols = plan.wide[0]
    cols = plan.chunk

    def project(k, step):
        at = pl.ds(pl.multiple_of(k * cols, LANES), step)
        qkv[:, at] = (product(normed[...], wall[:, at]) + qkv_bias[:, at]).astype(jnp.bfloat16)

    t = 3
    for early in range(t):
        tick(early)
    whole = qkv_cols // cols

    def qkv_step(k, carry):
        tick(k + t)
        finish(k)
        project(k, cols)
        return carry

    lax.fori_loop(0, whole, qkv_step, 0)
    t += whole
    done = whole
    if qkv_cols % cols:
        tick(t)
        finish(done)
        project(whole, qkv_cols % cols)
        t += 1
        done += 1

    head_size = plan.width // HEADS
    scale = head_size ** (-0.5) * math.log2(math.e)
    width = plan.width
    per_image = 2

    def attend(i, carry):
        at = pl.ds(pl.multiple_of(i * seq_pad, PACK), seq_pad)
        some = pl.ds(pl.multiple_of(i * seq_pad, PACK), seq)
        for head in range(HEADS):
            low = head * head_size
            q = qkv[at, low:low + head_size]
            k = qkv[some, width + low:width + low + head_size]
            v = qkv[some, 2 * width + low:2 * width + low + head_size]
            scores = lax.dot_general(q, k, (((1,), (1,)), ((), ())), preferred_element_type=jnp.float32)
            top = jnp.max(scores, axis=-1, keepdims=True)
            weights = jnp.exp2((scores - top) * scale)
            norm_by = 1.0 / jnp.sum(weights, axis=-1, keepdims=True)
            mixed[at, low:low + head_size] = (
                product(weights.astype(jnp.bfloat16), v) * norm_by).astype(jnp.bfloat16)
            if (head + 1) % (HEADS // per_image) == 0:
                tick(t + i * per_image + (head + 1) // (HEADS // per_image) - 1)
        return carry

    lax.fori_loop(0, plan.images, attend, 0)
    t += plan.images * per_image

    proj_last = -(-(plan.wide[0] + plan.wide[1]) // cols)
    while done < proj_last:
        while t < done + 3:
            tick(t)
            t += 1
        finish(done)
        done += 1
    at_proj = plan.wide[0]
    for low in range(0, width, 2 * LANES):
        high = min(low + 2 * LANES, width)
        resid[:, low:high] = (product(mixed[...], wall[:, at_proj + low:at_proj + high])
                              + proj_bias[:, low:high] + resid[:, low:high])
    norm(ln2_gain, ln2_bias)

    at_fc1 = plan.wide[0] + plan.wide[1]
    low = 0
    begun = done * cols - at_fc1
    pieces = []
    if begun:
        pieces.append((0, begun, None))
    at = begun
    for g in range(done, plan.col_chunks):
        pieces.append((at, at + cols, g))
        at += cols

    def up(low, high):
        pre = product(normed[...], wall[:, at_fc1 + low:at_fc1 + high]) + fc1_bias[:, low:high]
        qkv[:, low:high] = (pre * (1.0 + lax.erf(pre * math.sqrt(0.5))) * 0.5).astype(jnp.bfloat16)

    for count, (low, high, g) in enumerate(pieces):
        if g is not None:
            if count % 2 == 0 or t < g + 3:
                tick(t)
                t += 1
            while t < g + 3:
                tick(t)
                t += 1
            finish(g)
        up(low, high)

    hidden = plan.hidden
    writes = []
    for g in range(plan.col_chunks, plan.chunks):
        while t < g + 3 or (g == plan.chunks - 1 and t < plan.chunks + 2):
            tick(t)
            t += 1
        finish(g)
        for kind in plan.kinds:
            if kind[1] <= g < kind[2]:
                low = kind[4] + (g - kind[1]) * kind[3]
                high = low + kind[3]
        down = product(qkv[:, :hidden], wtwo[:, low:high]) + fc2_bias[:, low:high] + resid[:, low:high]
        down = down.astype(jnp.bfloat16)
        for i in range(plan.images):
            tok[i, :, low:high] = down[i * seq_pad:i * seq_pad + seq]
            write = pltpu.make_async_copy(
                tok.at[i, :, pl.ds(low, high - low)], out.at[i, :, pl.ds(low, high - low)],
                out_sem.at[g - plan.col_chunks, i])
            write.start()
            writes.append(write)
    for write in writes:
        write.wait()
    for phase in (Z, X1, Y1, X2, Y2, PART):
        def drain(g, carry, phase=phase):
            each_kind(g, lambda kind: wait_out(kind, phase))
            return carry
        lax.fori_loop(0, plan.chunks, drain, 0)


def fused(plan, tokens, weights, vectors):
    vmem = pl.BlockSpec(memory_space=pltpu.VMEM)
    anywhere = pl.BlockSpec(memory_space=pl.ANY)
    count = plan.chunks
    inner = max(plan.wide[0], plan.hidden)
    return pl.pallas_call(
        functools.partial(fused_kernel, plan),
        out_shape=jax.ShapeDtypeStruct(tokens.shape, jnp.bfloat16),
        in_specs=[anywhere] * 5 + [vmem] * len(vectors),
        out_specs=anywhere,
        scratch_shapes=[
            pltpu.VMEM((plan.ring * plan.depth, plan.total), jnp.bfloat16),
            pltpu.VMEM((plan.ring * plan.deep, plan.width), jnp.bfloat16),
            pltpu.VMEM(tokens.shape, jnp.bfloat16),
            pltpu.VMEM((plan.rows, plan.width), jnp.float32),
            pltpu.VMEM((plan.rows, plan.width), jnp.bfloat16),
            pltpu.VMEM((plan.rows, inner), jnp.bfloat16),
            pltpu.VMEM((plan.rows, plan.width), jnp.bfloat16),
            pltpu.SemaphoreType.DMA((6, count)),
            pltpu.SemaphoreType.DMA((6, count)),
            pltpu.SemaphoreType.DMA((5,)),
            pltpu.SemaphoreType.DMA((count - plan.col_chunks, plan.images)),
        ],
        compiler_params=pltpu.CompilerParams(
            collective_id=0, has_side_effects=True, vmem_limit_bytes=67_043_328),
    )(tokens, *weights, *vectors)


def gather(block):
    return lax.all_gather(block, "fsdp", axis=0, tiled=True)


def attend_kernel(head_size, q_ref, k_ref, v_ref, out_ref):
    scale = head_size ** (-0.5)
    for head in range(q_ref.shape[2] // head_size):
        at = slice(head * head_size, (head + 1) * head_size)
        scores = lax.dot_general(
            q_ref[0, :, at], k_ref[0, :, at], (((1,), (1,)), ((), ())),
            preferred_element_type=jnp.float32)
        top = jnp.max(scores, axis=-1, keepdims=True)
        weights = jnp.exp((scores - top) * scale)
        probs = weights / jnp.sum(weights, axis=-1, keepdims=True)
        mixed = product(probs.astype(jnp.bfloat16), v_ref[0, :, at])
        out_ref[0, :, at] = mixed.astype(jnp.bfloat16)


def attend(qkv, head_size):
    images, seq_len, wide = qkv.shape
    width = wide // 3
    spec = [
        pl.BlockSpec((1, seq_len, width), functools.partial(lambda part, i: (i, 0, part), part))
        for part in range(3)
    ]
    return pl.pallas_call(
        functools.partial(attend_kernel, head_size),
        grid=(images,),
        in_specs=spec,
        out_specs=pl.BlockSpec((1, seq_len, width), lambda i: (i, 0, 0)),
        out_shape=jax.ShapeDtypeStruct((images, seq_len, width), jnp.bfloat16),
        compiler_params=pltpu.CompilerParams(vmem_limit_bytes=48 * 1024 * 1024),
        cost_estimate=pl.CostEstimate(
            flops=4 * images * seq_len * seq_len * width,
            bytes_accessed=8 * images * seq_len * width,
            transcendentals=images * seq_len * seq_len * width // head_size,
        ),
    )(qkv, qkv, qkv)


def plain(tokens, ln1_gain, ln1_bias, qkv_weight, qkv_bias, proj_weight, proj_bias,
          ln2_gain, ln2_bias, fc1_weight, fc1_bias, fc2_weight, fc2_bias):
    images, seq_len, width = tokens.shape
    resid_input = tokens.reshape(-1, width).astype(jnp.float32)
    normed = layer_norm(resid_input, ln1_gain, ln1_bias).astype(jnp.bfloat16)
    qkv_sum = product(normed, gather(qkv_weight))
    qkv_proj = (qkv_sum + qkv_bias).astype(jnp.bfloat16).reshape(images, seq_len, 3 * width)
    attended = attend(qkv_proj, width // HEADS).reshape(-1, width)
    resid = product(attended, gather(proj_weight)) + proj_bias + resid_input
    normed_two = layer_norm(resid, ln2_gain, ln2_bias).astype(jnp.bfloat16)
    pre_act = product(normed_two, gather(fc1_weight))
    hidden = jax.nn.gelu(pre_act + fc1_bias, approximate=False).astype(jnp.bfloat16)
    result = product(hidden, gather(fc2_weight)) + fc2_bias + resid
    return result.astype(jnp.bfloat16).reshape(images, seq_len, width)


def on_device(tokens, ln1_gain, ln1_bias, qkv_weight, qkv_bias, proj_weight, proj_bias,
              ln2_gain, ln2_bias, fc1_weight, fc1_bias, fc2_weight, fc2_bias):
    weights = (qkv_weight, proj_weight, fc1_weight, fc2_weight)
    plan = Plan(lax.axis_size("dp"), lax.axis_size("fsdp"), tokens, weights)
    if not plan.fits:
        return plain(tokens, ln1_gain, ln1_bias, qkv_weight, qkv_bias, proj_weight, proj_bias,
                     ln2_gain, ln2_bias, fc1_weight, fc1_bias, fc2_weight, fc2_bias)
    vectors = (ln1_gain, ln1_bias, qkv_bias, proj_bias, ln2_gain, ln2_bias, fc1_bias, fc2_bias)
    return fused(plan, tokens, weights, [v.reshape(1, -1) for v in vectors])


def solution(mesh):
    whole, rows = P(), P("fsdp", None)
    split = P(("dp", "fsdp"), None, None)
    placed = (split, whole, whole, rows, whole, rows, whole, whole, whole, rows, whole, rows, whole)
    return jax.shard_map(on_device, mesh=mesh, in_specs=placed, out_specs=split, check_vma=False)
```

```python
import functools
import math
import jax
import jax.numpy as jnp
from jax import lax
from jax.experimental import pallas as pl
from jax.experimental.pallas import tpu as pltpu
from jax.sharding import PartitionSpec as P

HEADS = 16
LANES = 128
PACK = 16
EPS = 1e-06
AHEAD = 2


def layer_norm(values, gain, bias):
    average = jnp.mean(values, axis=-1, keepdims=True)
    centered = values - average
    variance = jnp.mean(centered * centered, axis=-1, keepdims=True)
    return centered * lax.rsqrt(variance + EPS) * gain + bias


def product(left, weight):
    return jnp.dot(left, weight, preferred_element_type=jnp.float32)


def round_up(value, step):
    return -(-value // step) * step


def row_block(rows, most):
    best = PACK
    for size in range(PACK, most + 1, PACK):
        if rows % size == 0:
            best = size
    return best


class Plan:
    def __init__(self, shares, ring, tokens, weights):
        self.shares, self.ring = shares, ring
        self.images, self.seq, self.width = tokens.shape
        qkv, proj, fc1, fc2 = weights
        self.depth = qkv.shape[0]
        self.deep = fc2.shape[0]
        self.wide = [w.shape[1] for w in (qkv, proj, fc1)]
        self.total = sum(self.wide)
        self.chunk = shares * LANES
        self.hidden = fc1.shape[1]
        self.seq_pad = round_up(self.seq, PACK)
        self.rows = self.images * self.seq_pad
        zs = ring // 2
        self.fits = (
            shares == 4
            and ring % 2 == 0
            and zs >= 4
            and zs & (zs - 1) == 0
            and self.depth % PACK == 0
            and self.deep % (shares * PACK) == 0
            and all(w % LANES == 0 for w in self.wide)
            and self.total % self.chunk == 0
            and self.width % LANES == 0
            and self.width >= self.chunk
            and self.wide[0] == 3 * self.width
            and self.width % HEADS == 0
        )
        if not self.fits:
            return
        self.narrow = 2 * LANES
        self.col_chunks = self.total // self.chunk
        self.kinds = [("col", 0, self.col_chunks, self.chunk, 0)]
        whole = self.width // self.narrow
        at = self.col_chunks
        self.kinds.append(("row", at, at + whole, self.narrow, 0))
        at += whole
        if self.width % self.narrow:
            self.kinds.append(("row", at, at + 1, self.width % self.narrow, whole * self.narrow))
            at += 1
        self.chunks = at
        self.groups = self.width // self.chunk
        self.rest = self.width % self.chunk
        self.segments = []
        for group in range(self.groups):
            for piece in range(3):
                self.segments.append((0, piece * self.width + group * self.chunk, self.chunk))
        for piece in range(3):
            if self.rest:
                self.segments.append((0, piece * self.width + self.groups * self.chunk, self.rest))
        self.segments.append((1, 0, self.wide[1]))
        self.segments.append((2, 0, self.wide[2]))
        kept = ring * (self.depth * self.total + self.deep * self.width) * 2
        acts = self.rows * (self.width * (4 + 2 + 2 + 2) + max(3 * self.width, self.hidden) * 2)
        self.fits = kept + acts < 58 * 1024 * 1024


def flip(value, mask):
    bit = 1
    while bit <= mask:
        if mask & bit:
            value = value + bit - 2 * bit * lax.rem(value // bit, 2)
        bit *= 2
    return value


def fused_kernel(plan, tokens, qkv_hbm, proj_hbm, fc1_hbm, fc2_hbm,
                 ln1_gain, ln1_bias, qkv_bias, proj_bias, ln2_gain, ln2_bias, fc1_bias, fc2_bias,
                 out, wall, wtwo, tok, resid, normed, qkv, mixed,
                 send_sem, recv_sem, own_sem, out_sem):
    shares, ring = plan.shares, plan.ring
    zs = ring // 2
    depth, deep = plan.depth, plan.deep
    rows, seq, seq_pad = plan.rows, plan.seq, plan.seq_pad
    share = lax.axis_index("dp")
    place = lax.axis_index("fsdp")
    z, core = place // 2, lax.rem(place, 2)
    Z, X1, Y1, X2, Y2, PART = range(6)
    side_x, side_y, corner = flip(share, 1), flip(share, 2), flip(share, 3)
    partner = flip(place, 1)
    near = flip(z, 1) * 2 + core
    far = [flip(z, mask) * 2 + core for mask in range(2, zs)]

    def device(d, f):
        return {"dp": d, "fsdp": f}

    def part(kind, who, block_share):
        name, first, _, cols, base, g = kind
        if name == "col":
            r = pl.multiple_of(who * depth, PACK)
            c = pl.multiple_of((g * shares + block_share) * LANES, LANES)
            return wall.at[pl.ds(r, depth), pl.ds(c, LANES)]
        size = deep // shares
        r = pl.multiple_of(who * deep + block_share * size, PACK)
        c = pl.multiple_of(base + (g - first) * cols, LANES)
        return wtwo.at[pl.ds(r, size), pl.ds(c, cols)]

    def entire(kind, who):
        name, first, _, cols, base, g = kind
        if name == "col":
            return wall.at[pl.ds(pl.multiple_of(who * depth, PACK), depth),
                           pl.ds(pl.multiple_of(g * cols, LANES), cols)]
        return wtwo.at[pl.ds(pl.multiple_of(who * deep, PACK), deep),
                       pl.ds(pl.multiple_of(base + (g - first) * cols, LANES), cols)]

    def copy(ref, phase, g, d, f):
        return pltpu.make_async_remote_copy(
            src_ref=ref, dst_ref=ref, send_sem=send_sem.at[phase, g], recv_sem=recv_sem.at[phase, g],
            device_id=device(d, f), device_id_type=pl.DeviceIdType.MESH)

    def volume(kind, phase):
        name, cols = kind[0], kind[3]
        ref = wall if name == "col" else wtwo
        if phase == PART:
            return ref.at[pl.ds(0, zs * (depth if name == "col" else deep)), pl.ds(0, cols)]
        blocks = {Z: zs, X1: zs - 1, Y1: zs - 1, X2: (zs - 2) // 2, Y2: (zs - 2) // 2}[phase]
        size, cols = (depth, LANES) if name == "col" else (deep // shares, cols)
        return ref.at[pl.ds(0, blocks * size), pl.ds(0, cols)]

    def wait_on(kind, phase, sems):
        region = volume(kind, phase)
        pltpu.make_async_copy(region, region, sems.at[phase, kind[5]]).wait()

    def each_kind(g, body):
        if isinstance(g, int):
            for kind in plan.kinds:
                if kind[1] <= g < kind[2]:
                    body(kind + (g,))
            return
        for kind in plan.kinds:
            @pl.when(jnp.logical_and(g >= kind[1], g < kind[2]))
            def _(kind=kind):
                body(kind + (g,))

    def send_z(g):
        def body(kind):
            mine = part(kind, place, share)
            for other in far:
                copy(mine, Z, g, share, other).start()
            copy(mine, Z, g, share, near).start()
            copy(part(kind, place, corner), Z, g, share, near).start()
        each_kind(g, body)

    def relay_a(g):
        def body(kind):
            wait_on(kind, Z, recv_sem)
            for other in far + [near]:
                block = part(kind, other, share)
                copy(block, X1, g, side_x, place).start()
                copy(block, Y1, g, side_y, place).start()
        each_kind(g, body)

    def relay_b(g):
        def body(kind):
            wait_on(kind, X1, recv_sem)
            wait_on(kind, Y1, recv_sem)
            for one, two in zip(far[0::2], far[1::2]):
                copy(part(kind, one, side_y), X2, g, side_x, place).start()
                copy(part(kind, two, side_x), Y2, g, side_y, place).start()
        each_kind(g, body)

    def relay_c(g):
        def body(kind):
            wait_on(kind, X2, recv_sem)
            wait_on(kind, Y2, recv_sem)
            for who in [place, near] + far:
                copy(entire(kind, who), PART, g, share, partner).start()
        each_kind(g, body)

    def finish(g):
        each_kind(g, lambda kind: wait_on(kind, PART, recv_sem))

    ahead = AHEAD

    def tick(t):
        for low, action in ((ahead, send_z), (0, relay_a), (-1, relay_b), (-2, relay_c)):
            if not isinstance(t, int) or 0 <= t + low < plan.chunks:
                action(t + low)

    own = []
    base = 0
    for at, (which, low, size) in enumerate(plan.segments):
        ref = (qkv_hbm, proj_hbm, fc1_hbm)[which]
        own.append((which, pltpu.make_async_copy(
            ref.at[:, pl.ds(low, size)],
            wall.at[pl.ds(pl.multiple_of(place * depth, PACK), depth), pl.ds(base, size)],
            own_sem.at[at])))
        base += size
    own.append((3, pltpu.make_async_copy(
        fc2_hbm, wtwo.at[pl.ds(pl.multiple_of(place * deep, PACK), deep), :],
        own_sem.at[len(plan.segments)])))
    token_copy = pltpu.make_async_copy(tokens, tok, own_sem.at[len(plan.segments) + 1])
    barrier = pltpu.get_barrier_semaphore()
    peers = [(share, other) for other in far + [near, partner]]
    peers += [(side_x, place), (side_y, place)]
    for d, f in peers:
        pl.semaphore_signal(barrier, inc=1, device_id=device(d, f), device_id_type=pl.DeviceIdType.MESH)
    for which, c in own[:-3]:
        c.start()
    token_copy.start()
    for which, c in own[-3:]:
        c.start()
    pl.semaphore_wait(barrier, len(peers))
    for g in range(ahead):
        own[g][1].wait()
        send_z(g)

    token_copy.wait()
    for i in range(plan.images):
        tail = seq_pad - PACK
        resid[pl.ds(i * seq_pad + tail, PACK), :] = jnp.zeros((PACK, plan.width), jnp.float32)
        resid[pl.ds(i * seq_pad, seq), :] = tok[i].astype(jnp.float32)
    block = row_block(rows, 64)

    def norm(gain, bias):
        def body(r, carry):
            at = pl.ds(pl.multiple_of(r * block, PACK), block)
            normed[at, :] = layer_norm(resid[at, :], gain[...], bias[...]).astype(jnp.bfloat16)
            return carry
        lax.fori_loop(0, rows // block, body, 0)

    norm(ln1_gain, ln1_bias)
    for which, c in own[ahead:]:
        c.wait()

    cols = plan.chunk
    width = plan.width
    head_size = width // HEADS
    scale = head_size ** (-0.5) * math.log2(math.e)

    def project(source, target, size):
        source = pl.multiple_of(source, LANES)
        target = pl.multiple_of(target, LANES)
        qkv[:, pl.ds(target, size)] = (
            product(normed[...], wall[:, pl.ds(source, size)]) + qkv_bias[pl.ds(target, size)]
        ).astype(jnp.bfloat16)

    def project_chunk(g):
        project(g * cols, lax.rem(g, 3) * width + g // 3 * cols, cols)

    def attend(i, heads):
        at = pl.ds(pl.multiple_of(i * seq_pad, PACK), seq_pad)
        some = pl.ds(pl.multiple_of(i * seq_pad, PACK), seq)
        for head in heads:
            low = head * head_size
            q = qkv[at, low:low + head_size]
            k = qkv[some, width + low:width + low + head_size]
            v = qkv[some, 2 * width + low:2 * width + low + head_size]
            scores = lax.dot_general(q, k, (((1,), (1,)), ((), ())), preferred_element_type=jnp.float32)
            top = jnp.max(scores, axis=-1, keepdims=True)
            weights = jnp.exp2((scores - top) * scale)
            norm_by = 1.0 / jnp.sum(weights, axis=-1, keepdims=True)
            mixed[at, low:low + head_size] = (
                product(weights.astype(jnp.bfloat16), v) * norm_by).astype(jnp.bfloat16)

    ready = [0] + [(g + 1) * cols // head_size for g in range(plan.groups)] + [HEADS]
    heads_of = [list(range(low, high)) for low, high in zip(ready, ready[1:])]

    clock = [0]
    last_tick = plan.chunks + 2

    def advance(to):
        while clock[0] < to:
            tick(clock[0])
            clock[0] += 1

    advance(3)
    t = clock[0]

    def first_chunks(g, carry):
        tick(g + t)
        finish(g)
        project_chunk(g)
        return carry

    lax.fori_loop(0, 3, first_chunks, 0)
    clock[0] += 3
    for group in range(1, plan.groups):
        t = clock[0]

        def both(i, carry, group=group, t=t):
            attend(i, heads_of[group - 1])
            tick(t + i)
            finish(group * 3 + i)
            project_chunk(group * 3 + i)
            return carry

        fused_steps = min(3, plan.images)
        lax.fori_loop(0, fused_steps, both, 0)
        clock[0] += fused_steps
        for i in range(fused_steps, 3):
            advance(clock[0] + 1)
            finish(group * 3 + i)
            project_chunk(group * 3 + i)
        if plan.images > fused_steps:
            def more(i, carry, group=group):
                attend(i, heads_of[group - 1])
                return carry
            lax.fori_loop(fused_steps, plan.images, more, 0)
    t = clock[0]
    last_whole = heads_of[plan.groups - 1]

    def middle(i, carry):
        attend(i, last_whole)
        tick(t + i)
        return carry

    lax.fori_loop(0, plan.images, middle, 0)
    clock[0] += plan.images
    done = 3 * plan.groups

    def complete(columns):
        nonlocal done
        while done * cols < columns:
            advance(done + 3)
            finish(done)
            done += 1

    if plan.rest:
        complete(plan.wide[0])
        for piece in range(3):
            project(3 * plan.groups * cols + piece * plan.rest,
                    piece * width + plan.groups * cols, plan.rest)
        advance(clock[0] + 1)
    if heads_of[plan.groups]:
        t = clock[0]

        def last(i, carry):
            attend(i, heads_of[plan.groups])
            tick(t + i)
            return carry

        lax.fori_loop(0, plan.images, last, 0)
        clock[0] += plan.images

    at_proj = plan.wide[0]
    complete(plan.wide[0] + plan.wide[1])
    for low in range(0, width, 2 * LANES):
        high = min(low + 2 * LANES, width)
        resid[:, low:high] = (product(mixed[...], wall[:, at_proj + low:at_proj + high])
                              + proj_bias[low:high] + resid[:, low:high])
    advance(clock[0] + 1)
    norm(ln2_gain, ln2_bias)
    advance(clock[0] + 1)

    at_fc1 = plan.wide[0] + plan.wide[1]
    bounds = [at_fc1] + list(range(round_up(at_fc1 + 1, cols), plan.total + 1, cols))
    for count, (low, high) in enumerate(zip(bounds, bounds[1:])):
        complete(high)
        pre = product(normed[...], wall[:, low:high]) + fc1_bias[low - at_fc1:high - at_fc1]
        qkv[:, low - at_fc1:high - at_fc1] = (
            pre * (1.0 + lax.erf(pre * math.sqrt(0.5))) * 0.5).astype(jnp.bfloat16)
        if count % 2:
            advance(min(clock[0] + 1, last_tick))

    hidden = plan.hidden
    writes = []
    for g in range(plan.col_chunks, plan.chunks):
        advance(g + 3)
        finish(g)
        for kind in plan.kinds:
            if kind[1] <= g < kind[2]:
                low = kind[4] + (g - kind[1]) * kind[3]
                high = low + kind[3]
        for i in range(plan.images):
            at = slice(i * seq_pad, (i + 1) * seq_pad)
            down = product(qkv[at, :hidden], wtwo[:, low:high]) + fc2_bias[low:high] + resid[at, low:high]
            tok[i, :, low:high] = down.astype(jnp.bfloat16)[:seq]
            write = pltpu.make_async_copy(
                tok.at[i, :, pl.ds(low, high - low)], out.at[i, :, pl.ds(low, high - low)],
                out_sem.at[g - plan.col_chunks, i])
            write.start()
            writes.append(write)
        advance(min(clock[0] + 1, last_tick))
        if g == plan.chunks - 2:
            for phase in (Z, X1, Y1, X2, Y2, PART):
                def drain(g, carry, phase=phase):
                    each_kind(g, lambda kind: wait_on(kind, phase, send_sem))
                    return carry
                lax.fori_loop(0, plan.chunks, drain, 0)
    for write in writes:
        write.wait()


def fused(plan, tokens, weights, vectors):
    vmem = pl.BlockSpec(memory_space=pltpu.VMEM)
    anywhere = pl.BlockSpec(memory_space=pl.ANY)
    count = plan.chunks
    inner = max(plan.wide[0], plan.hidden)
    return pl.pallas_call(
        functools.partial(fused_kernel, plan),
        out_shape=jax.ShapeDtypeStruct(tokens.shape, jnp.bfloat16),
        in_specs=[anywhere] * 5 + [vmem] * len(vectors),
        out_specs=anywhere,
        scratch_shapes=[
            pltpu.VMEM((plan.ring * plan.depth, plan.total), jnp.bfloat16),
            pltpu.VMEM((plan.ring * plan.deep, plan.width), jnp.bfloat16),
            pltpu.VMEM(tokens.shape, jnp.bfloat16),
            pltpu.VMEM((plan.rows, plan.width), jnp.float32),
            pltpu.VMEM((plan.rows, plan.width), jnp.bfloat16),
            pltpu.VMEM((plan.rows, inner), jnp.bfloat16),
            pltpu.VMEM((plan.rows, plan.width), jnp.bfloat16),
            pltpu.SemaphoreType.DMA((6, count)),
            pltpu.SemaphoreType.DMA((6, count)),
            pltpu.SemaphoreType.DMA((len(plan.segments) + 2,)),
            pltpu.SemaphoreType.DMA((count - plan.col_chunks, plan.images)),
        ],
        compiler_params=pltpu.CompilerParams(
            collective_id=0, has_side_effects=True, vmem_limit_bytes=67_043_328),
    )(tokens, *weights, *vectors)


def gather(block):
    return lax.all_gather(block, "fsdp", axis=0, tiled=True)


def attend_kernel(head_size, q_ref, k_ref, v_ref, out_ref):
    scale = head_size ** (-0.5)
    for head in range(q_ref.shape[2] // head_size):
        at = slice(head * head_size, (head + 1) * head_size)
        scores = lax.dot_general(
            q_ref[0, :, at], k_ref[0, :, at], (((1,), (1,)), ((), ())),
            preferred_element_type=jnp.float32)
        top = jnp.max(scores, axis=-1, keepdims=True)
        weights = jnp.exp((scores - top) * scale)
        probs = weights / jnp.sum(weights, axis=-1, keepdims=True)
        mixed = product(probs.astype(jnp.bfloat16), v_ref[0, :, at])
        out_ref[0, :, at] = mixed.astype(jnp.bfloat16)


def attend(qkv, head_size):
    images, seq_len, wide = qkv.shape
    width = wide // 3
    spec = [
        pl.BlockSpec((1, seq_len, width), functools.partial(lambda part, i: (i, 0, part), part))
        for part in range(3)
    ]
    return pl.pallas_call(
        functools.partial(attend_kernel, head_size),
        grid=(images,),
        in_specs=spec,
        out_specs=pl.BlockSpec((1, seq_len, width), lambda i: (i, 0, 0)),
        out_shape=jax.ShapeDtypeStruct((images, seq_len, width), jnp.bfloat16),
        compiler_params=pltpu.CompilerParams(vmem_limit_bytes=48 * 1024 * 1024),
        cost_estimate=pl.CostEstimate(
            flops=4 * images * seq_len * seq_len * width,
            bytes_accessed=8 * images * seq_len * width,
            transcendentals=images * seq_len * seq_len * width // head_size,
        ),
    )(qkv, qkv, qkv)


def plain(tokens, ln1_gain, ln1_bias, qkv_weight, qkv_bias, proj_weight, proj_bias,
          ln2_gain, ln2_bias, fc1_weight, fc1_bias, fc2_weight, fc2_bias):
    images, seq_len, width = tokens.shape
    resid_input = tokens.reshape(-1, width).astype(jnp.float32)
    normed = layer_norm(resid_input, ln1_gain, ln1_bias).astype(jnp.bfloat16)
    qkv_sum = product(normed, gather(qkv_weight))
    qkv_proj = (qkv_sum + qkv_bias).astype(jnp.bfloat16).reshape(images, seq_len, 3 * width)
    attended = attend(qkv_proj, width // HEADS).reshape(-1, width)
    resid = product(attended, gather(proj_weight)) + proj_bias + resid_input
    normed_two = layer_norm(resid, ln2_gain, ln2_bias).astype(jnp.bfloat16)
    pre_act = product(normed_two, gather(fc1_weight))
    hidden = jax.nn.gelu(pre_act + fc1_bias, approximate=False).astype(jnp.bfloat16)
    result = product(hidden, gather(fc2_weight)) + fc2_bias + resid
    return result.astype(jnp.bfloat16).reshape(images, seq_len, width)


def on_device(tokens, ln1_gain, ln1_bias, qkv_weight, qkv_bias, proj_weight, proj_bias,
              ln2_gain, ln2_bias, fc1_weight, fc1_bias, fc2_weight, fc2_bias):
    weights = (qkv_weight, proj_weight, fc1_weight, fc2_weight)
    plan = Plan(lax.axis_size("dp"), lax.axis_size("fsdp"), tokens, weights)
    if not plan.fits:
        return plain(tokens, ln1_gain, ln1_bias, qkv_weight, qkv_bias, proj_weight, proj_bias,
                     ln2_gain, ln2_bias, fc1_weight, fc1_bias, fc2_weight, fc2_bias)
    vectors = (ln1_gain, ln1_bias, qkv_bias, proj_bias, ln2_gain, ln2_bias, fc1_bias, fc2_bias)
    return fused(plan, tokens, weights, vectors)


def solution(mesh):
    whole, rows = P(), P("fsdp", None)
    split = P(("dp", "fsdp"), None, None)
    placed = (split, whole, whole, rows, whole, rows, whole, whole, whole, rows, whole, rows, whole)
    return jax.shard_map(on_device, mesh=mesh, in_specs=placed, out_specs=split, check_vma=False)
```

```python
import functools
import math
import jax
import jax.numpy as jnp
from jax import lax
from jax.experimental import pallas as pl
from jax.experimental.pallas import tpu as pltpu
from jax.sharding import PartitionSpec as P

HEADS = 16
LANES = 128
PACK = 16
EPS = 1e-06
AHEAD = 2


def layer_norm(values, gain, bias):
    average = jnp.mean(values, axis=-1, keepdims=True)
    centered = values - average
    variance = jnp.mean(centered * centered, axis=-1, keepdims=True)
    return centered * lax.rsqrt(variance + EPS) * gain + bias


def product(left, weight):
    return jnp.dot(left, weight, preferred_element_type=jnp.float32)


def round_up(value, step):
    return -(-value // step) * step


class Plan:
    def __init__(self, shares, ring, tokens, weights):
        self.shares, self.ring = shares, ring
        self.images, self.seq, self.width = tokens.shape
        qkv, proj, fc1, fc2 = weights
        self.depth = qkv.shape[0]
        self.deep = fc2.shape[0]
        self.wide = [w.shape[1] for w in (qkv, proj, fc1)]
        self.total = sum(self.wide)
        self.chunk = shares * LANES
        self.hidden = fc1.shape[1]
        self.seq_pad = round_up(self.seq, PACK)
        self.rows = self.images * self.seq_pad
        zs = ring // 2
        self.fits = (
            shares == 4
            and ring % 2 == 0
            and zs >= 4
            and zs & (zs - 1) == 0
            and self.depth % PACK == 0
            and self.deep % (shares * PACK) == 0
            and all(w % LANES == 0 for w in self.wide)
            and self.total % self.chunk == 0
            and self.width % LANES == 0
            and self.width >= self.chunk
            and self.wide[0] == 3 * self.width
            and self.width % HEADS == 0
        )
        if not self.fits:
            return
        self.narrow = 2 * LANES
        self.col_chunks = self.total // self.chunk
        self.kinds = [("col", 0, self.col_chunks, self.chunk, 0)]
        whole = self.width // self.narrow
        at = self.col_chunks
        self.kinds.append(("row", at, at + whole, self.narrow, 0))
        at += whole
        if self.width % self.narrow:
            self.kinds.append(("row", at, at + 1, self.width % self.narrow, whole * self.narrow))
            at += 1
        self.chunks = at
        self.groups = self.width // self.chunk
        self.rest = self.width % self.chunk
        self.segments = []
        for group in range(self.groups):
            for piece in range(3):
                self.segments.append((0, piece * self.width + group * self.chunk, self.chunk))
        for piece in range(3):
            if self.rest:
                self.segments.append((0, piece * self.width + self.groups * self.chunk, self.rest))
        self.segments.append((1, 0, self.wide[1]))
        self.segments.append((2, 0, self.wide[2]))
        kept = ring * (self.depth * self.total + self.deep * self.width) * 2
        acts = self.rows * (self.width * (4 + 2 + 2 + 2) + max(3 * self.width, self.hidden) * 2)
        self.fits = kept + acts < 58 * 1024 * 1024


def flip(value, mask):
    bit = 1
    while bit <= mask:
        if mask & bit:
            value = value + bit - 2 * bit * lax.rem(value // bit, 2)
        bit *= 2
    return value


def fused_kernel(plan, tokens, qkv_hbm, proj_hbm, fc1_hbm, fc2_hbm,
                 *rest):
    vectors, out, held = rest[:8], rest[8], rest[9:17]
    wall, wtwo, tok, resid, normed, qkv, mixed, send_sem, recv_sem, own_sem, out_sem, vec_sem = rest[17:]
    ln1_gain, ln1_bias, qkv_bias, proj_bias, ln2_gain, ln2_bias, fc1_bias, fc2_bias = held
    shares, ring = plan.shares, plan.ring
    zs = ring // 2
    depth, deep = plan.depth, plan.deep
    rows, seq, seq_pad = plan.rows, plan.seq, plan.seq_pad
    share = lax.axis_index("dp")
    place = lax.axis_index("fsdp")
    z, core = place // 2, lax.rem(place, 2)
    Z, X1, Y1, X2, Y2, PART = range(6)
    side_x, side_y, corner = flip(share, 1), flip(share, 2), flip(share, 3)
    partner = flip(place, 1)
    near = flip(z, 1) * 2 + core
    far = [flip(z, mask) * 2 + core for mask in range(2, zs)]

    def device(d, f):
        return {"dp": d, "fsdp": f}

    def part(kind, who, block_share):
        name, first, _, cols, base, g = kind
        if name == "col":
            r = pl.multiple_of(who * depth, PACK)
            c = pl.multiple_of((g * shares + block_share) * LANES, LANES)
            return wall.at[pl.ds(r, depth), pl.ds(c, LANES)]
        size = deep // shares
        r = pl.multiple_of(who * deep + block_share * size, PACK)
        c = pl.multiple_of(base + (g - first) * cols, LANES)
        return wtwo.at[pl.ds(r, size), pl.ds(c, cols)]

    def entire(kind, who):
        name, first, _, cols, base, g = kind
        if name == "col":
            return wall.at[pl.ds(pl.multiple_of(who * depth, PACK), depth),
                           pl.ds(pl.multiple_of(g * cols, LANES), cols)]
        return wtwo.at[pl.ds(pl.multiple_of(who * deep, PACK), deep),
                       pl.ds(pl.multiple_of(base + (g - first) * cols, LANES), cols)]

    def copy(ref, phase, kind, d, f):
        g, form = kind[5], int(kind[0] == "row")
        return pltpu.make_async_remote_copy(
            src_ref=ref, dst_ref=ref, send_sem=send_sem.at[phase, form], recv_sem=recv_sem.at[phase, g],
            device_id=device(d, f), device_id_type=pl.DeviceIdType.MESH)

    blocks_of = {Z: zs, X1: zs - 1, Y1: zs - 1, X2: (zs - 2) // 2, Y2: (zs - 2) // 2}

    def volume(kind, phase):
        name, cols = kind[0], kind[3]
        ref = wall if name == "col" else wtwo
        if phase == PART:
            return ref.at[pl.ds(0, zs * (depth if name == "col" else deep)), pl.ds(0, cols)]
        count = blocks_of[phase]
        size, cols = (depth, LANES) if name == "col" else (deep // shares, cols)
        return ref.at[pl.ds(0, count * size), pl.ds(0, cols)]

    def totals(phase):
        if phase == PART:
            return wall.at[pl.ds(0, zs * depth), :], wtwo.at[pl.ds(0, zs * deep), :]
        count = blocks_of[phase]
        return (wall.at[pl.ds(0, count * depth), pl.ds(0, plan.col_chunks * LANES)],
                wtwo.at[pl.ds(0, count * (deep // shares)), :])

    def wait_on(kind, phase):
        region = volume(kind, phase)
        pltpu.make_async_copy(region, region, recv_sem.at[phase, kind[5]]).wait()

    def each_kind(g, body):
        if isinstance(g, int):
            for kind in plan.kinds:
                if kind[1] <= g < kind[2]:
                    body(kind + (g,))
            return
        for kind in plan.kinds:
            @pl.when(jnp.logical_and(g >= kind[1], g < kind[2]))
            def _(kind=kind):
                body(kind + (g,))

    def send_z(g):
        def body(kind):
            mine = part(kind, place, share)
            for other in far:
                copy(mine, Z, kind, share, other).start()
            copy(mine, Z, kind, share, near).start()
            copy(part(kind, place, corner), Z, kind, share, near).start()
        each_kind(g, body)

    def relay_a(g):
        def body(kind):
            wait_on(kind, Z)
            for other in far + [near]:
                block = part(kind, other, share)
                copy(block, X1, kind, side_x, place).start()
                copy(block, Y1, kind, side_y, place).start()
        each_kind(g, body)

    def relay_b(g):
        def body(kind):
            wait_on(kind, X1)
            wait_on(kind, Y1)
            for one, two in zip(far[0::2], far[1::2]):
                copy(part(kind, one, side_y), X2, kind, side_x, place).start()
                copy(part(kind, two, side_x), Y2, kind, side_y, place).start()
        each_kind(g, body)

    def relay_c(g):
        def body(kind):
            wait_on(kind, X2)
            wait_on(kind, Y2)
            for who in [place, near] + far:
                copy(entire(kind, who), PART, kind, share, partner).start()
        each_kind(g, body)

    def finish(g):
        each_kind(g, lambda kind: wait_on(kind, PART))

    ahead = AHEAD

    def act(t, steps):
        for low, action in steps:
            if not isinstance(t, int) or 0 <= t + low < plan.chunks:
                action(t + low)

    def tick_one(t):
        act(t, ((ahead, send_z), (-3, relay_c), (0, relay_a)))

    def tick_two(t):
        act(t, ((-1, relay_b),))

    def tick(t):
        tick_one(t)
        tick_two(t)

    own = []
    base = 0
    for at, (which, low, size) in enumerate(plan.segments):
        ref = (qkv_hbm, proj_hbm, fc1_hbm)[which]
        own.append((which, pltpu.make_async_copy(
            ref.at[:, pl.ds(low, size)],
            wall.at[pl.ds(pl.multiple_of(place * depth, PACK), depth), pl.ds(base, size)],
            own_sem.at[at])))
        base += size
    own.append((3, pltpu.make_async_copy(
        fc2_hbm, wtwo.at[pl.ds(pl.multiple_of(place * deep, PACK), deep), :],
        own_sem.at[len(plan.segments)])))
    token_copy = pltpu.make_async_copy(tokens, tok, own_sem.at[len(plan.segments) + 1])
    barrier = pltpu.get_barrier_semaphore()
    peers = [(share, other) for other in far + [near, partner]]
    peers += [(side_x, place), (side_y, place)]
    for d, f in peers:
        pl.semaphore_signal(barrier, inc=1, device_id=device(d, f), device_id_type=pl.DeviceIdType.MESH)
    for which, c in own[:ahead]:
        c.start()
    token_copy.start()
    vector_copies = [
        pltpu.make_async_copy(source, target, vec_sem.at[at])
        for at, (source, target) in enumerate(zip(vectors, held))]
    for c in vector_copies:
        c.start()
    for which, c in own[ahead:]:
        c.start()
    pl.semaphore_wait(barrier, len(peers))
    for g in range(ahead):
        own[g][1].wait()
        send_z(g)

    token_copy.wait()
    for i in range(plan.images):
        tail = seq_pad - PACK
        resid[pl.ds(i * seq_pad + tail, PACK), :] = jnp.zeros((PACK, plan.width), jnp.float32)
        resid[pl.ds(i * seq_pad, seq), :] = tok[i].astype(jnp.float32)
    block = seq_pad

    def norm(gain, bias, low, high):
        def body(r, carry):
            at = pl.ds(pl.multiple_of(r * block, PACK), block)
            normed[at, :] = layer_norm(resid[at, :], gain[...], bias[...]).astype(jnp.bfloat16)
            return carry
        lax.fori_loop(low, high, body, 0)

    blocks = rows // block
    for c in vector_copies:
        c.wait()
    norm(ln1_gain, ln1_bias, 0, blocks)
    for which, c in own[ahead:]:
        c.wait()

    cols = plan.chunk
    width = plan.width
    head_size = width // HEADS
    scale = head_size ** (-0.5) * math.log2(math.e)

    def project(source, target, size):
        source = pl.multiple_of(source, LANES)
        target = pl.multiple_of(target, LANES)
        qkv[:, pl.ds(target, size)] = (
            product(normed[...], wall[:, pl.ds(source, size)]) + qkv_bias[pl.ds(target, size)]
        ).astype(jnp.bfloat16)

    def project_chunk(g):
        project(g * cols, lax.rem(g, 3) * width + g // 3 * cols, cols)

    def attend(i, heads):
        at = pl.ds(pl.multiple_of(i * seq_pad, PACK), seq_pad)
        some = pl.ds(pl.multiple_of(i * seq_pad, PACK), seq)
        for head in heads:
            low = head * head_size
            q = qkv[at, low:low + head_size]
            k = qkv[some, width + low:width + low + head_size]
            v = qkv[some, 2 * width + low:2 * width + low + head_size]
            scores = lax.dot_general(k, q, (((1,), (1,)), ((), ())), preferred_element_type=jnp.float32)
            top = jnp.max(scores, axis=0, keepdims=True)
            weights = jnp.exp2((scores - top) * scale)
            norm_by = 1.0 / jnp.sum(weights, axis=0, keepdims=True)
            out_t = lax.dot_general(v, weights.astype(jnp.bfloat16), (((0,), (0,)), ((), ())),
                                    preferred_element_type=jnp.float32) * norm_by
            mixed[at, low:low + head_size] = out_t.T.astype(jnp.bfloat16)

    def attend_ticking(i, heads, t):
        tick_one(t)
        attend(i, heads[:len(heads) // 2])
        tick_two(t)
        attend(i, heads[len(heads) // 2:])

    ready = [0] + [(g + 1) * cols // head_size for g in range(plan.groups)] + [HEADS]
    heads_of = [list(range(low, high)) for low, high in zip(ready, ready[1:])]

    clock = [0, 0]
    last_tick = plan.chunks + 3

    def half():
        if clock[0] < last_tick:
            (tick_two if clock[1] else tick_one)(clock[0])
            clock[0] += clock[1]
            clock[1] = 1 - clock[1]

    def advance(to):
        while clock[0] < to:
            half()

    def reach(g):
        while clock[0] < g + 3 or (clock[0] == g + 3 and not clock[1]):
            half()

    advance(3)
    t = clock[0]

    def first_chunks(g, carry):
        tick(g + t)
        finish(g)
        project_chunk(g)
        return carry

    lax.fori_loop(0, 3, first_chunks, 0)
    clock[0] += 3
    for group in range(1, plan.groups):
        t = clock[0]

        def both(i, carry, group=group, t=t):
            tick_one(t + i)
            attend(i, heads_of[group - 1])
            tick_two(t + i)
            finish(group * 3 + i)
            project_chunk(group * 3 + i)
            return carry

        fused_steps = min(3, plan.images)
        lax.fori_loop(0, fused_steps, both, 0)
        clock[0] += fused_steps
        for i in range(fused_steps, 3):
            advance(clock[0] + 1)
            finish(group * 3 + i)
            project_chunk(group * 3 + i)
        if plan.images > fused_steps:
            def more(i, carry, group=group):
                attend(i, heads_of[group - 1])
                return carry
            lax.fori_loop(fused_steps, plan.images, more, 0)
    t = clock[0]
    last_whole = heads_of[plan.groups - 1]

    def middle(i, carry):
        attend_ticking(i, last_whole, t + i)
        return carry

    lax.fori_loop(0, plan.images, middle, 0)
    clock[0] += plan.images
    done = 3 * plan.groups

    def complete(columns):
        nonlocal done
        while done * cols < columns:
            reach(done)
            finish(done)
            done += 1

    if plan.rest:
        complete(plan.wide[0])
        for piece in range(3):
            project(3 * plan.groups * cols + piece * plan.rest,
                    piece * width + plan.groups * cols, plan.rest)
            if piece < 2:
                half()
    if heads_of[plan.groups]:
        t = clock[0]

        def last(i, carry):
            attend_ticking(i, heads_of[plan.groups], t + i)
            return carry

        lax.fori_loop(0, plan.images, last, 0)
        clock[0] += plan.images

    at_proj = plan.wide[0]
    complete(plan.wide[0] + plan.wide[1])
    half()
    for low in range(0, width, 2 * LANES):
        high = min(low + 2 * LANES, width)
        resid[:, low:high] = (product(mixed[...], wall[:, at_proj + low:at_proj + high])
                              + proj_bias[low:high] + resid[:, low:high])
        if low <= width // 2 < high:
            half()
    half()
    norm(ln2_gain, ln2_bias, 0, blocks // 2)
    half()
    norm(ln2_gain, ln2_bias, blocks // 2, blocks)
    half()

    at_fc1 = plan.wide[0] + plan.wide[1]
    bounds = [at_fc1] + list(range(round_up(at_fc1 + 1, cols), plan.total + 1, cols))
    for count, (low, high) in enumerate(zip(bounds, bounds[1:])):
        complete(high)
        pre = product(normed[...], wall[:, low:high]) + fc1_bias[low - at_fc1:high - at_fc1]
        qkv[:, low - at_fc1:high - at_fc1] = (
            pre * (1.0 + lax.erf(pre * math.sqrt(0.5))) * 0.5).astype(jnp.bfloat16)
        half()

    hidden = plan.hidden
    writes = []
    for g in range(plan.col_chunks, plan.chunks, 2):
        final = min(g + 2, plan.chunks)
        for each in range(g, final):
            reach(each)
            finish(each)
        low = (g - plan.col_chunks) * plan.narrow
        high = min(low + (final - g) * plan.narrow, width)
        for i in range(plan.images):
            at = slice(i * seq_pad, (i + 1) * seq_pad)
            down = product(qkv[at, :hidden], wtwo[:, low:high]) + fc2_bias[low:high] + resid[at, low:high]
            tok[i, :, low:high] = down.astype(jnp.bfloat16)[:seq]
            write = pltpu.make_async_copy(
                tok.at[i, :, pl.ds(low, high - low)], out.at[i, :, pl.ds(low, high - low)],
                out_sem.at[g - plan.col_chunks, i])
            write.start()
            writes.append(write)
            half()
        if final == plan.chunks:
            for phase in (Z, X1, Y1, X2, Y2, PART):
                for form, region in enumerate(totals(phase)):
                    pltpu.make_async_copy(region, region, send_sem.at[phase, form]).wait()
    for write in writes:
        write.wait()


def fused(plan, tokens, weights, vectors):
    anywhere = pl.BlockSpec(memory_space=pl.ANY)
    count = plan.chunks
    inner = max(plan.wide[0], plan.hidden)
    return pl.pallas_call(
        functools.partial(fused_kernel, plan),
        out_shape=jax.ShapeDtypeStruct(tokens.shape, jnp.bfloat16),
        in_specs=[anywhere] * (5 + len(vectors)),
        out_specs=anywhere,
        scratch_shapes=[pltpu.VMEM(v.shape, v.dtype) for v in vectors] + [
            pltpu.VMEM((plan.ring * plan.depth, plan.total), jnp.bfloat16),
            pltpu.VMEM((plan.ring * plan.deep, plan.width), jnp.bfloat16),
            pltpu.VMEM(tokens.shape, jnp.bfloat16),
            pltpu.VMEM((plan.rows, plan.width), jnp.float32),
            pltpu.VMEM((plan.rows, plan.width), jnp.bfloat16),
            pltpu.VMEM((plan.rows, inner), jnp.bfloat16),
            pltpu.VMEM((plan.rows, plan.width), jnp.bfloat16),
            pltpu.SemaphoreType.DMA((6, 2)),
            pltpu.SemaphoreType.DMA((6, count)),
            pltpu.SemaphoreType.DMA((len(plan.segments) + 2,)),
            pltpu.SemaphoreType.DMA((count - plan.col_chunks, plan.images)),
            pltpu.SemaphoreType.DMA((len(vectors),)),
        ],
        compiler_params=pltpu.CompilerParams(
            collective_id=0, has_side_effects=True, vmem_limit_bytes=67_043_328),
    )(tokens, *weights, *vectors)


def gather(block):
    return lax.all_gather(block, "fsdp", axis=0, tiled=True)


def attend_kernel(head_size, q_ref, k_ref, v_ref, out_ref):
    scale = head_size ** (-0.5)
    for head in range(q_ref.shape[2] // head_size):
        at = slice(head * head_size, (head + 1) * head_size)
        scores = lax.dot_general(
            q_ref[0, :, at], k_ref[0, :, at], (((1,), (1,)), ((), ())),
            preferred_element_type=jnp.float32)
        top = jnp.max(scores, axis=-1, keepdims=True)
        weights = jnp.exp((scores - top) * scale)
        probs = weights / jnp.sum(weights, axis=-1, keepdims=True)
        mixed = product(probs.astype(jnp.bfloat16), v_ref[0, :, at])
        out_ref[0, :, at] = mixed.astype(jnp.bfloat16)


def attend(qkv, head_size):
    images, seq_len, wide = qkv.shape
    width = wide // 3
    spec = [
        pl.BlockSpec((1, seq_len, width), functools.partial(lambda part, i: (i, 0, part), part))
        for part in range(3)
    ]
    return pl.pallas_call(
        functools.partial(attend_kernel, head_size),
        grid=(images,),
        in_specs=spec,
        out_specs=pl.BlockSpec((1, seq_len, width), lambda i: (i, 0, 0)),
        out_shape=jax.ShapeDtypeStruct((images, seq_len, width), jnp.bfloat16),
        compiler_params=pltpu.CompilerParams(vmem_limit_bytes=48 * 1024 * 1024),
        cost_estimate=pl.CostEstimate(
            flops=4 * images * seq_len * seq_len * width,
            bytes_accessed=8 * images * seq_len * width,
            transcendentals=images * seq_len * seq_len * width // head_size,
        ),
    )(qkv, qkv, qkv)


def plain(tokens, ln1_gain, ln1_bias, qkv_weight, qkv_bias, proj_weight, proj_bias,
          ln2_gain, ln2_bias, fc1_weight, fc1_bias, fc2_weight, fc2_bias):
    images, seq_len, width = tokens.shape
    resid_input = tokens.reshape(-1, width).astype(jnp.float32)
    normed = layer_norm(resid_input, ln1_gain, ln1_bias).astype(jnp.bfloat16)
    qkv_sum = product(normed, gather(qkv_weight))
    qkv_proj = (qkv_sum + qkv_bias).astype(jnp.bfloat16).reshape(images, seq_len, 3 * width)
    attended = attend(qkv_proj, width // HEADS).reshape(-1, width)
    resid = product(attended, gather(proj_weight)) + proj_bias + resid_input
    normed_two = layer_norm(resid, ln2_gain, ln2_bias).astype(jnp.bfloat16)
    pre_act = product(normed_two, gather(fc1_weight))
    hidden = jax.nn.gelu(pre_act + fc1_bias, approximate=False).astype(jnp.bfloat16)
    result = product(hidden, gather(fc2_weight)) + fc2_bias + resid
    return result.astype(jnp.bfloat16).reshape(images, seq_len, width)


def on_device(tokens, ln1_gain, ln1_bias, qkv_weight, qkv_bias, proj_weight, proj_bias,
              ln2_gain, ln2_bias, fc1_weight, fc1_bias, fc2_weight, fc2_bias):
    weights = (qkv_weight, proj_weight, fc1_weight, fc2_weight)
    plan = Plan(lax.axis_size("dp"), lax.axis_size("fsdp"), tokens, weights)
    if not plan.fits:
        return plain(tokens, ln1_gain, ln1_bias, qkv_weight, qkv_bias, proj_weight, proj_bias,
                     ln2_gain, ln2_bias, fc1_weight, fc1_bias, fc2_weight, fc2_bias)
    vectors = (ln1_gain, ln1_bias, qkv_bias, proj_bias, ln2_gain, ln2_bias, fc1_bias, fc2_bias)
    return fused(plan, tokens, weights, vectors)


def solution(mesh):
    whole, rows = P(), P("fsdp", None)
    split = P(("dp", "fsdp"), None, None)
    placed = (split, whole, whole, rows, whole, rows, whole, whole, whole, rows, whole, rows, whole)
    return jax.shard_map(on_device, mesh=mesh, in_specs=placed, out_specs=split, check_vma=False)
```

```python
import functools
import math
import jax
import jax.numpy as jnp
from jax import lax
from jax.experimental import pallas as pl
from jax.experimental.pallas import tpu as pltpu
from jax.sharding import PartitionSpec as P

HEADS = 16
LANES = 128
PACK = 16
EPS = 1e-06
AHEAD = 2


def layer_norm(values, gain, bias):
    average = jnp.mean(values, axis=-1, keepdims=True)
    centered = values - average
    variance = jnp.mean(centered * centered, axis=-1, keepdims=True)
    return centered * lax.rsqrt(variance + EPS) * gain + bias


def product(left, weight):
    return jnp.dot(left, weight, preferred_element_type=jnp.float32)


def round_up(value, step):
    return -(-value // step) * step


class Plan:
    def __init__(self, shares, ring, tokens, weights):
        self.shares, self.ring = shares, ring
        self.images, self.seq, self.width = tokens.shape
        qkv, proj, fc1, fc2 = weights
        self.depth = qkv.shape[0]
        self.deep = fc2.shape[0]
        self.wide = [w.shape[1] for w in (qkv, proj, fc1)]
        self.total = sum(self.wide)
        self.chunk = shares * LANES
        self.hidden = fc1.shape[1]
        self.seq_pad = round_up(self.seq, PACK)
        self.rows = self.images * self.seq_pad
        zs = ring // 2
        self.fits = (
            shares == 4
            and ring % 2 == 0
            and zs >= 4
            and zs & (zs - 1) == 0
            and self.depth % PACK == 0
            and self.deep % (shares * PACK) == 0
            and all(w % LANES == 0 for w in self.wide)
            and self.total % self.chunk == 0
            and self.width % LANES == 0
            and self.width >= self.chunk
            and self.wide[0] == 3 * self.width
            and self.width % HEADS == 0
        )
        if not self.fits:
            return
        self.narrow = 2 * LANES
        self.col_chunks = self.total // self.chunk
        self.kinds = [("col", 0, self.col_chunks, self.chunk, 0)]
        whole = self.width // self.narrow
        at = self.col_chunks
        self.kinds.append(("row", at, at + whole, self.narrow, 0))
        at += whole
        if self.width % self.narrow:
            self.kinds.append(("row", at, at + 1, self.width % self.narrow, whole * self.narrow))
            at += 1
        self.chunks = at
        self.groups = self.width // self.chunk
        self.rest = self.width % self.chunk
        self.segments = []
        for group in range(self.groups):
            for piece in range(3):
                self.segments.append((0, piece * self.width + group * self.chunk, self.chunk))
        for piece in range(3):
            if self.rest:
                self.segments.append((0, piece * self.width + self.groups * self.chunk, self.rest))
        self.segments.append((1, 0, self.wide[1]))
        self.segments.append((2, 0, self.wide[2]))
        kept = ring * (self.depth * self.total + self.deep * self.width) * 2
        acts = self.rows * (self.width * (4 + 2 + 2 + 2) + max(3 * self.width, self.hidden) * 2)
        self.fits = kept + acts < 58 * 1024 * 1024


def flip(value, mask):
    bit = 1
    while bit <= mask:
        if mask & bit:
            value = value + bit - 2 * bit * lax.rem(value // bit, 2)
        bit *= 2
    return value


def fused_kernel(plan, tokens, qkv_hbm, proj_hbm, fc1_hbm, fc2_hbm,
                 *rest):
    vectors, out, held = rest[:8], rest[8], rest[9:17]
    wall, wtwo, tok, resid, normed, qkv, mixed, send_sem, recv_sem, own_sem, out_sem, vec_sem = rest[17:]
    ln1_gain, ln1_bias, qkv_bias, proj_bias, ln2_gain, ln2_bias, fc1_bias, fc2_bias = held
    shares, ring = plan.shares, plan.ring
    zs = ring // 2
    depth, deep = plan.depth, plan.deep
    rows, seq, seq_pad = plan.rows, plan.seq, plan.seq_pad
    share = lax.axis_index("dp")
    place = lax.axis_index("fsdp")
    z, core = place // 2, lax.rem(place, 2)
    Z, X1, Y1, X2, Y2, PART = range(6)
    side_x, side_y, corner = flip(share, 1), flip(share, 2), flip(share, 3)
    partner = flip(place, 1)
    near = flip(z, 1) * 2 + core
    far = [flip(z, mask) * 2 + core for mask in range(2, zs)]

    def device(d, f):
        return {"dp": d, "fsdp": f}

    def part(kind, who, block_share):
        name, first, _, cols, base, g = kind
        if name == "col":
            r = pl.multiple_of(who * depth, PACK)
            c = pl.multiple_of((g * shares + block_share) * LANES, LANES)
            return wall.at[pl.ds(r, depth), pl.ds(c, LANES)]
        size = deep // shares
        r = pl.multiple_of(who * deep + block_share * size, PACK)
        c = pl.multiple_of(base + (g - first) * cols, LANES)
        return wtwo.at[pl.ds(r, size), pl.ds(c, cols)]

    def entire(kind, who):
        name, first, _, cols, base, g = kind
        if name == "col":
            return wall.at[pl.ds(pl.multiple_of(who * depth, PACK), depth),
                           pl.ds(pl.multiple_of(g * cols, LANES), cols)]
        return wtwo.at[pl.ds(pl.multiple_of(who * deep, PACK), deep),
                       pl.ds(pl.multiple_of(base + (g - first) * cols, LANES), cols)]

    def copy(ref, phase, kind, d, f):
        g, form = kind[5], int(kind[0] == "row")
        return pltpu.make_async_remote_copy(
            src_ref=ref, dst_ref=ref, send_sem=send_sem.at[phase, form], recv_sem=recv_sem.at[phase, g],
            device_id=device(d, f), device_id_type=pl.DeviceIdType.MESH)

    blocks_of = {Z: zs, X1: zs - 1, Y1: zs - 1, X2: (zs - 2) // 2, Y2: (zs - 2) // 2}

    def volume(kind, phase):
        name, cols = kind[0], kind[3]
        ref = wall if name == "col" else wtwo
        if phase == PART:
            return ref.at[pl.ds(0, zs * (depth if name == "col" else deep)), pl.ds(0, cols)]
        count = blocks_of[phase]
        size, cols = (depth, LANES) if name == "col" else (deep // shares, cols)
        return ref.at[pl.ds(0, count * size), pl.ds(0, cols)]

    def totals(phase):
        if phase == PART:
            return wall.at[pl.ds(0, zs * depth), :], wtwo.at[pl.ds(0, zs * deep), :]
        count = blocks_of[phase]
        return (wall.at[pl.ds(0, count * depth), pl.ds(0, plan.col_chunks * LANES)],
                wtwo.at[pl.ds(0, count * (deep // shares)), :])

    def wait_on(kind, phase):
        region = volume(kind, phase)
        pltpu.make_async_copy(region, region, recv_sem.at[phase, kind[5]]).wait()

    def each_kind(g, body):
        if isinstance(g, int):
            for kind in plan.kinds:
                if kind[1] <= g < kind[2]:
                    body(kind + (g,))
            return
        for kind in plan.kinds:
            @pl.when(jnp.logical_and(g >= kind[1], g < kind[2]))
            def _(kind=kind):
                body(kind + (g,))

    def send_z(g):
        def body(kind):
            mine = part(kind, place, share)
            for other in far:
                copy(mine, Z, kind, share, other).start()
            copy(mine, Z, kind, share, near).start()
            copy(part(kind, place, corner), Z, kind, share, near).start()
        each_kind(g, body)

    def relay_a(g):
        def body(kind):
            wait_on(kind, Z)
            for other in far + [near]:
                block = part(kind, other, share)
                copy(block, X1, kind, side_x, place).start()
                copy(block, Y1, kind, side_y, place).start()
        each_kind(g, body)

    def relay_b(g):
        def body(kind):
            wait_on(kind, X1)
            wait_on(kind, Y1)
            for one, two in zip(far[0::2], far[1::2]):
                copy(part(kind, one, side_y), X2, kind, side_x, place).start()
                copy(part(kind, two, side_x), Y2, kind, side_y, place).start()
        each_kind(g, body)

    def relay_c(g):
        def body(kind):
            wait_on(kind, X2)
            wait_on(kind, Y2)
            for who in [place, near] + far:
                copy(entire(kind, who), PART, kind, share, partner).start()
        each_kind(g, body)

    def finish(g):
        each_kind(g, lambda kind: wait_on(kind, PART))

    ahead = AHEAD

    def act(t, steps):
        for low, action in steps:
            if not isinstance(t, int) or 0 <= t + low < plan.chunks:
                action(t + low)

    def tick_one(t):
        act(t, ((ahead, send_z), (-3, relay_c), (0, relay_a)))

    def tick_two(t):
        act(t, ((-1, relay_b),))

    def tick(t):
        tick_one(t)
        tick_two(t)

    own = []
    base = 0
    for at, (which, low, size) in enumerate(plan.segments):
        ref = (qkv_hbm, proj_hbm, fc1_hbm)[which]
        own.append((which, pltpu.make_async_copy(
            ref.at[:, pl.ds(low, size)],
            wall.at[pl.ds(pl.multiple_of(place * depth, PACK), depth), pl.ds(base, size)],
            own_sem.at[at])))
        base += size
    own.append((3, pltpu.make_async_copy(
        fc2_hbm, wtwo.at[pl.ds(pl.multiple_of(place * deep, PACK), deep), :],
        own_sem.at[len(plan.segments)])))
    token_copy = pltpu.make_async_copy(tokens, tok, own_sem.at[len(plan.segments) + 1])
    barrier = pltpu.get_barrier_semaphore()
    peers = [(share, other) for other in far + [near, partner]]
    peers += [(side_x, place), (side_y, place)]
    for d, f in peers:
        pl.semaphore_signal(barrier, inc=1, device_id=device(d, f), device_id_type=pl.DeviceIdType.MESH)
    for which, c in own[:ahead]:
        c.start()
    token_copy.start()
    vector_copies = [
        pltpu.make_async_copy(source, target, vec_sem.at[at])
        for at, (source, target) in enumerate(zip(vectors, held))]
    for c in vector_copies:
        c.start()
    for which, c in own[ahead:]:
        c.start()
    pl.semaphore_wait(barrier, len(peers))
    for g in range(ahead):
        own[g][1].wait()
        send_z(g)

    token_copy.wait()
    for i in range(plan.images):
        tail = seq_pad - PACK
        resid[pl.ds(i * seq_pad + tail, PACK), :] = jnp.zeros((PACK, plan.width), jnp.float32)
        resid[pl.ds(i * seq_pad, seq), :] = tok[i].astype(jnp.float32)
    block = seq_pad

    def norm(gain, bias, low, high):
        def body(r, carry):
            at = pl.ds(pl.multiple_of(r * block, PACK), block)
            normed[at, :] = layer_norm(resid[at, :], gain[...], bias[...]).astype(jnp.bfloat16)
            return carry
        lax.fori_loop(low, high, body, 0)

    blocks = rows // block
    for c in vector_copies:
        c.wait()
    norm(ln1_gain, ln1_bias, 0, blocks)
    for which, c in own[ahead:]:
        c.wait()

    cols = plan.chunk
    width = plan.width
    head_size = width // HEADS
    scale = head_size ** (-0.5) * math.log2(math.e)

    def project(source, target, size):
        source = pl.multiple_of(source, LANES)
        target = pl.multiple_of(target, LANES)
        qkv[:, pl.ds(target, size)] = (
            product(normed[...], wall[:, pl.ds(source, size)]) + qkv_bias[pl.ds(target, size)]
        ).astype(jnp.bfloat16)

    def project_chunk(g):
        project(g * cols, lax.rem(g, 3) * width + g // 3 * cols, cols)

    def attend(i, heads):
        at = pl.ds(pl.multiple_of(i * seq_pad, PACK), seq_pad)
        some = pl.ds(pl.multiple_of(i * seq_pad, PACK), seq)
        for head in heads:
            low = head * head_size
            q = qkv[at, low:low + head_size]
            k = qkv[some, width + low:width + low + head_size]
            v = qkv[some, 2 * width + low:2 * width + low + head_size]
            scores = lax.dot_general(k, q, (((1,), (1,)), ((), ())), preferred_element_type=jnp.float32)
            top = jnp.max(scores, axis=0, keepdims=True)
            weights = jnp.exp2((scores - top) * scale)
            norm_by = 1.0 / jnp.sum(weights, axis=0, keepdims=True)
            out_t = lax.dot_general(v, weights.astype(jnp.bfloat16), (((0,), (0,)), ((), ())),
                                    preferred_element_type=jnp.float32) * norm_by
            mixed[at, low:low + head_size] = out_t.T.astype(jnp.bfloat16)

    def attend_ticking(i, heads, t):
        tick_one(t)
        attend(i, heads[:len(heads) // 2])
        tick_two(t)
        attend(i, heads[len(heads) // 2:])

    ready = [0] + [(g + 1) * cols // head_size for g in range(plan.groups)] + [HEADS]
    heads_of = [list(range(low, high)) for low, high in zip(ready, ready[1:])]

    clock = [0, 0]
    last_tick = plan.chunks + 3

    def half():
        if clock[0] < last_tick:
            (tick_two if clock[1] else tick_one)(clock[0])
            clock[0] += clock[1]
            clock[1] = 1 - clock[1]

    def advance(to):
        while clock[0] < to:
            half()

    def reach(g):
        while clock[0] < g + 3 or (clock[0] == g + 3 and not clock[1]):
            half()

    advance(3)
    t = clock[0]

    def first_chunks(g, carry):
        tick(g + t)
        finish(g)
        project_chunk(g)
        return carry

    lax.fori_loop(0, 3, first_chunks, 0)
    clock[0] += 3
    for group in range(1, plan.groups):
        t = clock[0]

        def both(i, carry, group=group, t=t):
            tick_one(t + i)
            attend(i, heads_of[group - 1])
            tick_two(t + i)
            finish(group * 3 + i)
            project_chunk(group * 3 + i)
            return carry

        fused_steps = min(3, plan.images)
        lax.fori_loop(0, fused_steps, both, 0)
        clock[0] += fused_steps
        for i in range(fused_steps, 3):
            advance(clock[0] + 1)
            finish(group * 3 + i)
            project_chunk(group * 3 + i)
        if plan.images > fused_steps:
            def more(i, carry, group=group):
                attend(i, heads_of[group - 1])
                return carry
            lax.fori_loop(fused_steps, plan.images, more, 0)
    t = clock[0]
    last_whole = heads_of[plan.groups - 1]

    def middle(i, carry):
        attend_ticking(i, last_whole, t + i)
        return carry

    lax.fori_loop(0, plan.images, middle, 0)
    clock[0] += plan.images
    done = 3 * plan.groups

    def complete(columns):
        nonlocal done
        while done * cols < columns:
            reach(done)
            finish(done)
            done += 1

    if plan.rest:
        complete(plan.wide[0])
        for piece in range(3):
            project(3 * plan.groups * cols + piece * plan.rest,
                    piece * width + plan.groups * cols, plan.rest)
            if piece < 2:
                half()
    if heads_of[plan.groups]:
        t = clock[0]

        def last(i, carry):
            attend_ticking(i, heads_of[plan.groups], t + i)
            return carry

        lax.fori_loop(0, plan.images, last, 0)
        clock[0] += plan.images

    at_proj = plan.wide[0]
    complete(plan.wide[0] + plan.wide[1])
    half()
    for low in range(0, width, 2 * LANES):
        high = min(low + 2 * LANES, width)
        resid[:, low:high] = (product(mixed[...], wall[:, at_proj + low:at_proj + high])
                              + proj_bias[low:high] + resid[:, low:high])
        if low <= width // 2 < high:
            half()
    half()
    norm(ln2_gain, ln2_bias, 0, blocks // 2)
    half()
    norm(ln2_gain, ln2_bias, blocks // 2, blocks)
    half()

    at_fc1 = plan.wide[0] + plan.wide[1]
    bounds = [at_fc1] + list(range(round_up(at_fc1 + 1, cols), plan.total + 1, cols))
    for count, (low, high) in enumerate(zip(bounds, bounds[1:])):
        complete(high)
        pre = product(normed[...], wall[:, low:high]) + fc1_bias[low - at_fc1:high - at_fc1]
        qkv[:, low - at_fc1:high - at_fc1] = (
            pre * (1.0 + lax.erf(pre * math.sqrt(0.5))) * 0.5).astype(jnp.bfloat16)
        half()

    hidden = plan.hidden
    writes = []
    starts = [g for g in range(plan.col_chunks, plan.chunks - 2, 2)]
    starts += [g for g in range(plan.chunks - 2, plan.chunks) if g not in starts]
    for g, final in zip(starts, starts[1:] + [plan.chunks]):
        for each in range(g, final):
            reach(each)
            finish(each)
        low = (g - plan.col_chunks) * plan.narrow
        high = min(low + (final - g) * plan.narrow, width)
        for i in range(plan.images):
            at = slice(i * seq_pad, (i + 1) * seq_pad)
            down = product(qkv[at, :hidden], wtwo[:, low:high]) + fc2_bias[low:high] + resid[at, low:high]
            tok[i, :, low:high] = down.astype(jnp.bfloat16)[:seq]
            write = pltpu.make_async_copy(
                tok.at[i, :, pl.ds(low, high - low)], out.at[i, :, pl.ds(low, high - low)],
                out_sem.at[g - plan.col_chunks, i])
            write.start()
            writes.append(write)
            half()
        if final == plan.chunks:
            for phase in (Z, X1, Y1, X2, Y2, PART):
                for form, region in enumerate(totals(phase)):
                    pltpu.make_async_copy(region, region, send_sem.at[phase, form]).wait()
    for write in writes:
        write.wait()


def fused(plan, tokens, weights, vectors):
    anywhere = pl.BlockSpec(memory_space=pl.ANY)
    count = plan.chunks
    inner = max(plan.wide[0], plan.hidden)
    return pl.pallas_call(
        functools.partial(fused_kernel, plan),
        out_shape=jax.ShapeDtypeStruct(tokens.shape, jnp.bfloat16),
        in_specs=[anywhere] * (5 + len(vectors)),
        out_specs=anywhere,
        scratch_shapes=[pltpu.VMEM(v.shape, v.dtype) for v in vectors] + [
            pltpu.VMEM((plan.ring * plan.depth, plan.total), jnp.bfloat16),
            pltpu.VMEM((plan.ring * plan.deep, plan.width), jnp.bfloat16),
            pltpu.VMEM(tokens.shape, jnp.bfloat16),
            pltpu.VMEM((plan.rows, plan.width), jnp.float32),
            pltpu.VMEM((plan.rows, plan.width), jnp.bfloat16),
            pltpu.VMEM((plan.rows, inner), jnp.bfloat16),
            pltpu.VMEM((plan.rows, plan.width), jnp.bfloat16),
            pltpu.SemaphoreType.DMA((6, 2)),
            pltpu.SemaphoreType.DMA((6, count)),
            pltpu.SemaphoreType.DMA((len(plan.segments) + 2,)),
            pltpu.SemaphoreType.DMA((count - plan.col_chunks, plan.images)),
            pltpu.SemaphoreType.DMA((len(vectors),)),
        ],
        compiler_params=pltpu.CompilerParams(
            collective_id=0, has_side_effects=True, vmem_limit_bytes=67_043_328),
    )(tokens, *weights, *vectors)


def gather(block):
    return lax.all_gather(block, "fsdp", axis=0, tiled=True)


def attend_kernel(head_size, q_ref, k_ref, v_ref, out_ref):
    scale = head_size ** (-0.5)
    for head in range(q_ref.shape[2] // head_size):
        at = slice(head * head_size, (head + 1) * head_size)
        scores = lax.dot_general(
            q_ref[0, :, at], k_ref[0, :, at], (((1,), (1,)), ((), ())),
            preferred_element_type=jnp.float32)
        top = jnp.max(scores, axis=-1, keepdims=True)
        weights = jnp.exp((scores - top) * scale)
        probs = weights / jnp.sum(weights, axis=-1, keepdims=True)
        mixed = product(probs.astype(jnp.bfloat16), v_ref[0, :, at])
        out_ref[0, :, at] = mixed.astype(jnp.bfloat16)


def attend(qkv, head_size):
    images, seq_len, wide = qkv.shape
    width = wide // 3
    spec = [
        pl.BlockSpec((1, seq_len, width), functools.partial(lambda part, i: (i, 0, part), part))
        for part in range(3)
    ]
    return pl.pallas_call(
        functools.partial(attend_kernel, head_size),
        grid=(images,),
        in_specs=spec,
        out_specs=pl.BlockSpec((1, seq_len, width), lambda i: (i, 0, 0)),
        out_shape=jax.ShapeDtypeStruct((images, seq_len, width), jnp.bfloat16),
        compiler_params=pltpu.CompilerParams(vmem_limit_bytes=48 * 1024 * 1024),
        cost_estimate=pl.CostEstimate(
            flops=4 * images * seq_len * seq_len * width,
            bytes_accessed=8 * images * seq_len * width,
            transcendentals=images * seq_len * seq_len * width // head_size,
        ),
    )(qkv, qkv, qkv)


def plain(tokens, ln1_gain, ln1_bias, qkv_weight, qkv_bias, proj_weight, proj_bias,
          ln2_gain, ln2_bias, fc1_weight, fc1_bias, fc2_weight, fc2_bias):
    images, seq_len, width = tokens.shape
    resid_input = tokens.reshape(-1, width).astype(jnp.float32)
    normed = layer_norm(resid_input, ln1_gain, ln1_bias).astype(jnp.bfloat16)
    qkv_sum = product(normed, gather(qkv_weight))
    qkv_proj = (qkv_sum + qkv_bias).astype(jnp.bfloat16).reshape(images, seq_len, 3 * width)
    attended = attend(qkv_proj, width // HEADS).reshape(-1, width)
    resid = product(attended, gather(proj_weight)) + proj_bias + resid_input
    normed_two = layer_norm(resid, ln2_gain, ln2_bias).astype(jnp.bfloat16)
    pre_act = product(normed_two, gather(fc1_weight))
    hidden = jax.nn.gelu(pre_act + fc1_bias, approximate=False).astype(jnp.bfloat16)
    result = product(hidden, gather(fc2_weight)) + fc2_bias + resid
    return result.astype(jnp.bfloat16).reshape(images, seq_len, width)


def on_device(tokens, ln1_gain, ln1_bias, qkv_weight, qkv_bias, proj_weight, proj_bias,
              ln2_gain, ln2_bias, fc1_weight, fc1_bias, fc2_weight, fc2_bias):
    weights = (qkv_weight, proj_weight, fc1_weight, fc2_weight)
    plan = Plan(lax.axis_size("dp"), lax.axis_size("fsdp"), tokens, weights)
    if not plan.fits:
        return plain(tokens, ln1_gain, ln1_bias, qkv_weight, qkv_bias, proj_weight, proj_bias,
                     ln2_gain, ln2_bias, fc1_weight, fc1_bias, fc2_weight, fc2_bias)
    vectors = (ln1_gain, ln1_bias, qkv_bias, proj_bias, ln2_gain, ln2_bias, fc1_bias, fc2_bias)
    return fused(plan, tokens, weights, vectors)


def solution(mesh):
    whole, rows = P(), P("fsdp", None)
    split = P(("dp", "fsdp"), None, None)
    placed = (split, whole, whole, rows, whole, rows, whole, whole, whole, rows, whole, rows, whole)
    return jax.shard_map(on_device, mesh=mesh, in_specs=placed, out_specs=split, check_vma=False)
```
